32 devices in a mesh: robot: 8 (over z, x), sub: 4 (over y, core).
Axes of the slice: x: 2, y: 2, z: 4, core: 2. Of those that a mesh axis runs over, the one named last changes fastest.
Arguments:
- landmark_copies: float32 [8, 4, 3, 512], P('robot', 'sub'), may hold values from -6 to 6
- dual_copies: float32 [8, 4, 3, 512], P('robot', 'sub'), may hold values from -4 to 4
- visibility: int32 [8, 4, 512], P('robot', 'sub'), may hold values from 0 to 511
- block_counts: int32 [8, 4, 8], P('robot', 'sub'), may hold values from 1 to 64, as said below
- consensus_old: float32 [8, 4, 3, 512], P('robot', 'sub'), may hold values from -6 to 6
- poses: float32 [8, 4, 6, 1024], P('robot', 'sub'), may hold values from -6 to 6
- inverse_blocks: float32 [8, 4, 36, 1024], P('robot', 'sub'), may hold values from -1.8 to 1.8
- jacobians: float32 [8, 4, 18, 4096], P('robot', 'sub'), may hold values from -3 to 3
- measurements: float32 [8, 4, 3, 4096], P('robot', 'sub'), may hold values from -6 to 6
- obs_pose: int32 [8, 4, 4096], P('robot', 'sub'), may hold values from 0 to 1023
- obs_slot: int32 [8, 4, 4096], P('robot', 'sub'), may hold values from 0 to 511, as said below
- edge_to: int32 [8, 4, 1024], P('robot', 'sub'), may hold values from 0 to 4095
- edge_offset: float32 [8, 4, 6, 1024], P('robot', 'sub'), may hold values from -3 to 3
Outputs:
- refined_poses: float32 [8, 4, 6, 1024], P('robot', 'sub')
- consensus: float32 [8, 4, 3, 512], P('robot', 'sub')
- dual_new: float32 [8, 4, 3, 512], P('robot', 'sub')
- residual_norms: float32 [2], replicated
The draws below stay inside these ranges and needn't reach their ends.
Inputs may be any that keep to these rules, and one draw needn't show every extreme that they name: block_counts[r,s,d] counts the live slots at the head of block d; for every sub index some robot receives full blocks from every robot, which robot varies with the draw. `obs_slot`: each observation names a live slot of its own device.
All inputs are finite; a program needn't handle non-finite values.
Results may differ from the reference program's by a relative error of at most 0.0001.
Values sent between devices are 32-bit elements; how exact they have to be, the bound alone decides.
A program may use at most 64 MiB of HBM per device.

```python
import math
import jax
import jax.numpy as jnp
import numpy as np
from jax import lax

LM_DEV = 512
CAP = 64
POSE_DEV = 1024
OBS_DEV = 4096
SLOTS = 512
POSES = 4096
N_ROBOT = 8
N_SUB = 4


def count_table(key):
    base = jax.random.randint(jax.random.fold_in(key, 11), (N_ROBOT, N_SUB, N_ROBOT), 1, CAP // 2 + 1)
    heavy = jax.random.randint(jax.random.fold_in(key, 12), (1, N_SUB, 1), 0, N_ROBOT)
    target = jnp.arange(N_ROBOT, dtype=jnp.int32)[None, None, :]
    return jnp.where(target == heavy, CAP, base).astype(jnp.int32)


def draw_block_counts(key, part):
    return count_table(key)


def draw_obs_slot(key, part):
    counts = count_table(key)
    blocks = jax.random.randint(jax.random.fold_in(key, 13), (N_ROBOT, N_SUB, OBS_DEV), 0, N_ROBOT)
    picks = jax.random.randint(jax.random.fold_in(key, 14), (N_ROBOT, N_SUB, OBS_DEV), 0, CAP)
    limit = jnp.take_along_axis(counts, blocks, axis=2)
    return (blocks * CAP + picks % limit).astype(jnp.int32)


def with_ends(result, rng, least, high):
    dims = result.shape
    place = [jax.random.randint(jax.random.fold_in(rng, axis), (), 0, dims[axis]) for axis in range(len(dims))]
    result = result.at[tuple(place)].set(least)
    longest = dims.index(max(dims))
    place[longest] = (place[longest] + 1) % dims[longest]
    return result.at[tuple(place)].set(high)


def block_scale(rng, extent, cuts, least, largest):
    loudness, own = 1.0, jax.random.fold_in(rng, 6)
    for axis_at, shards_of in cuts:
        heights = jnp.exp(jax.random.uniform(jax.random.fold_in(own, axis_at), (shards_of,), jnp.float32, least / len(cuts), largest / len(cuts)))
        loudness = loudness * jnp.repeat(heights, extent[axis_at] // shards_of).reshape([-1 if axis == axis_at else 1 for axis in range(len(extent))])
    return loudness


def rank_table(amount, lean):
    portions = [(1 << 20) // math.isqrt(standing ** lean) + 1 for standing in range(1, amount + 1)]
    scale = 1 + sum(portions) // (1 << 30)
    return np.cumsum(np.array([max(1, weight // scale) for weight in portions]))


def skewed_ids(rng, dims, number_of, lean):
    table = rank_table(number_of, lean)
    ticket = jax.random.randint(jax.random.fold_in(rng, 1), dims, 0, int(table[number_of - 1]))
    standing = jnp.searchsorted(jnp.asarray(table, jnp.int32), ticket, side="right")
    return jax.random.permutation(jax.random.fold_in(rng, 2), number_of)[standing].astype(jnp.int32)


def scatter_about(stream_key, extent, width, bound, split=(), kind=jnp.bfloat16):
    values = width * jax.random.normal(stream_key, extent, jnp.float32)
    if split:
        values = values * block_scale(stream_key, extent, split, -0.22, 0.18)
    return jnp.clip(values, -bound, bound).astype(kind)


def setup_inputs(seed: int = 0) -> dict:
    key_list = jax.random.split(jax.random.key(seed), 14)
    landmark_copies = scatter_about(key_list[0], (N_ROBOT, N_SUB, 3, SLOTS), 1.0, 6.0, ((0, 8), (1, 4)), jnp.float32)
    dual_copies = scatter_about(key_list[1], (N_ROBOT, N_SUB, 3, SLOTS), 0.5, 4.0, ((0, 8), (1, 4)), jnp.float32)
    visibility = with_ends(skewed_ids(key_list[2], (N_ROBOT, N_SUB, SLOTS), LM_DEV, 2), jax.random.fold_in(key_list[2], 3), 0, LM_DEV - 1).astype(jnp.int32)
    block_counts = draw_block_counts(jax.random.fold_in(key_list[13], 71), 0)
    consensus_old = scatter_about(key_list[4], (N_ROBOT, N_SUB, 3, LM_DEV), 1.0, 6.0, ((0, 8), (1, 4)), jnp.float32)
    poses = scatter_about(key_list[5], (N_ROBOT, N_SUB, 6, POSE_DEV), 1.0, 6.0, ((0, 8), (1, 4)), jnp.float32)
    inverse_blocks = scatter_about(key_list[6], (N_ROBOT, N_SUB, 36, POSE_DEV), 0.3, 1.8, ((0, 8), (1, 4)), jnp.float32)
    jacobians = scatter_about(key_list[7], (N_ROBOT, N_SUB, 18, OBS_DEV), 0.5, 3.0, ((0, 8), (1, 4)), jnp.float32)
    measurements = scatter_about(key_list[8], (N_ROBOT, N_SUB, 3, OBS_DEV), 1.0, 6.0, ((0, 8), (1, 4)), jnp.float32)
    obs_pose = with_ends(jax.random.randint(key_list[9], (N_ROBOT, N_SUB, OBS_DEV), 0, POSE_DEV), jax.random.fold_in(key_list[9], 1), 0, POSE_DEV - 1).astype(jnp.int32)
    obs_slot = draw_obs_slot(jax.random.fold_in(key_list[13], 71), 0)
    edge_to = with_ends(jax.random.randint(key_list[11], (N_ROBOT, N_SUB, POSE_DEV), 0, POSES), jax.random.fold_in(key_list[11], 1), 0, POSES - 1).astype(jnp.int32)
    edge_offset = scatter_about(key_list[12], (N_ROBOT, N_SUB, 6, POSE_DEV), 0.5, 3.0, ((0, 8), (1, 4)), jnp.float32)
    return {"landmark_copies": landmark_copies, "dual_copies": dual_copies, "visibility": visibility, "block_counts": block_counts, "consensus_old": consensus_old, "poses": poses, "inverse_blocks": inverse_blocks, "jacobians": jacobians, "measurements": measurements, "obs_pose": obs_pose, "obs_slot": obs_slot, "edge_to": edge_to, "edge_offset": edge_offset}


penalty = 2.0

def reference(landmark_copies, dual_copies, visibility, block_counts, consensus_old, poses, inverse_blocks, jacobians, measurements, obs_pose, obs_slot, edge_to, edge_offset):
    robots = N_ROBOT
    subs = N_SUB
    live_mask = (jnp.arange(CAP)[None, None, None, :] < block_counts[..., None]).reshape(robots, subs, SLOTS).astype(jnp.float32)
    outgoing = (landmark_copies + dual_copies) * live_mask[:, :, None, :]
    target = (jnp.arange(SLOTS, dtype=jnp.int32) // CAP)[None, None, :] * LM_DEV + visibility
    sum_list = []
    seen_list = []
    for sub_index in range(subs):
        values = jnp.moveaxis(outgoing[:, sub_index], 1, 0).reshape(3, robots * SLOTS)
        flat_ids = target[:, sub_index].reshape(robots * SLOTS).astype(jnp.int32)
        summed = jax.vmap(lambda entries: jax.ops.segment_sum(entries, flat_ids, num_segments=robots * LM_DEV))(values)
        sum_list.append(jnp.moveaxis(summed.reshape(3, robots, LM_DEV), 0, 1))
        counted = jax.ops.segment_sum(live_mask[:, sub_index].reshape(robots * SLOTS), flat_ids, num_segments=robots * LM_DEV)
        seen_list.append(counted.reshape(robots, LM_DEV))
    totals = jnp.stack(sum_list, axis=1)
    seen = jnp.stack(seen_list, axis=1)
    consensus = (consensus_old + totals) / (1.0 + seen[:, :, None, :])
    back_list = []
    for sub_index in range(subs):
        flat = jnp.moveaxis(consensus[:, sub_index], 1, 0).reshape(3, robots * LM_DEV)
        picked = flat[:, target[:, sub_index]]
        back_list.append(jnp.moveaxis(picked, 1, 0))
    back = jnp.stack(back_list, axis=1)
    differ = (landmark_copies - back) * live_mask[:, :, None, :]
    dual_new = dual_copies + differ
    primal = jnp.sum(differ * differ)
    change = consensus - consensus_old
    dualsum = penalty * penalty * jnp.sum(seen[:, :, None, :] * change * change)
    residual_norms = jnp.sqrt(jnp.stack([primal, dualsum]) / (LM_DEV * robots * subs))
    copies_at = jnp.take_along_axis(landmark_copies, obs_slot[:, :, None, :], axis=3)
    error = measurements - copies_at
    jac_rows = jacobians.reshape(robots, subs, 3, 6, OBS_DEV)
    pull = lax.optimization_barrier(jnp.sum(jac_rows * error[:, :, :, None, :], axis=2))

    def pose_sums(rows, pose_ids):
        return jax.vmap(lambda entries: jax.ops.segment_sum(entries, pose_ids, num_segments=POSE_DEV))(rows)
    grad_obs = jax.vmap(jax.vmap(pose_sums))(pull, obs_pose)
    robot_all = jnp.moveaxis(poses, 1, 2).reshape(robots, 6, subs * POSE_DEV)
    pose_far = jax.vmap(lambda table, where: table[:, where])(robot_all, edge_to.reshape(robots, subs * POSE_DEV))
    pose_far = jnp.moveaxis(pose_far.reshape(robots, 6, subs, POSE_DEV), 2, 1)
    grad = grad_obs + pose_far - poses - edge_offset
    inverse = inverse_blocks.reshape(robots, subs, 6, 6, POSE_DEV)
    delta = lax.optimization_barrier(jnp.sum(inverse * grad[:, :, None, :, :], axis=3))
    return (poses + delta, consensus, dual_new, residual_norms)
```

```python
import functools

import jax
import jax.numpy as jnp
from jax import lax
from jax.experimental import pallas as pl
from jax.experimental.pallas import tpu as pltpu
from jax.sharding import PartitionSpec as P

penalty = 2.0
LANES = 128
CHUNK = 8
MESH = pl.DeviceIdType.MESH
f32, bf16, i32 = jnp.float32, jnp.bfloat16, jnp.int32


def pieces(x):
    hi = x.astype(bf16).astype(f32)
    return hi, x - hi


def pad_rows(x, rows):
    return jnp.concatenate([x, jnp.zeros((rows - x.shape[0], x.shape[1]), x.dtype)], axis=0)


def strip(ref, first, count, tiles, start, length, at=()):
    parts = [
        ref[(*at, pl.ds(first * tiles + t, count, stride=tiles), slice(None))] if count > 1
        else ref[(*at, slice(first * tiles + t, first * tiles + t + 1), slice(None))]
        for t in range(start, start + length)
    ]
    return parts[0] if length == 1 else jnp.concatenate(parts, axis=1)


def stack_rows(ref, t):
    return jnp.concatenate([ref[k, t : t + 1, :] for k in range(ref.shape[0])], axis=0)


def one_hot(lo):
    rows = lax.broadcasted_iota(i32, (LANES, lo.shape[1]), 0)
    return jnp.where(rows == lo, 1.0, 0.0).astype(bf16)


def table(x, width):
    groups = []
    for h in range(x.shape[1] // width):
        hi, lo = pieces(pad_rows(x[:, h * width : (h + 1) * width], 8))
        groups.append(jnp.concatenate([hi, lo], axis=1))
    return jnp.concatenate(groups, axis=0).astype(bf16)


def pick(tab, hot, hi):
    found = jnp.dot(tab, jnp.concatenate([hot, hot], axis=0), preferred_element_type=f32)
    total = None
    for h in range(tab.shape[0] // 8):
        part = jnp.where(hi == h, found[h * 8 : h * 8 + 8], 0.0)
        total = part if total is None else total + part
    return total


def spread(values, hot, hi, tiles):
    a, b = pieces(values)
    both = jnp.concatenate([a, b], axis=0)
    lhs = jnp.concatenate([jnp.where(hi == h, both, 0.0) for h in range(tiles)], axis=0).astype(bf16)
    return lax.dot_general(lhs, hot, (((1,), (1,)), ((), ())), preferred_element_type=f32)


def kernel(
    robots, subs,
    copies_ref, duals_ref, vis_ref, counts_ref, old_ref, poses_ref, inv_ref, jac_ref, meas_ref,
    obs_pose_ref, obs_slot_ref, edge_to_ref, edge_off_ref,
    refined_ref, cons_ref, dual_ref, res_ref,
    outgoing, received, back_out, back_in, pose_in, part_out, part_in,
    send1, recv1, send2, recv2, sendp, recvp, send3, recv3,
):
    me_r = lax.axis_index("robot")
    me_s = lax.axis_index("sub")
    slot_tiles = vis_ref.shape[0]
    slots = slot_tiles * LANES
    block = slots // robots
    per = LANES // block
    tiles = old_ref.shape[1]
    owned = tiles * LANES
    pose_tiles = edge_to_ref.shape[0]
    obs_tiles = obs_slot_ref.shape[0]
    params = poses_ref.shape[0] // pose_tiles

    barrier = pltpu.get_barrier_semaphore()
    for k in range(1, robots):
        pl.semaphore_signal(barrier, inc=1, device_id={"robot": lax.rem(me_r + k, robots)}, device_id_type=MESH)
    for k in range(1, subs):
        pl.semaphore_signal(barrier, inc=1, device_id={"sub": lax.rem(me_s + k, subs)}, device_id_type=MESH)

    lane = lax.broadcasted_iota(i32, (1, LANES), 1)
    copies = jnp.concatenate([stack_rows(copies_ref, t) for t in range(slot_tiles)], axis=1)
    for t in range(slots // LANES):
        cut = slice(t * LANES, (t + 1) * LANES)
        base = jnp.concatenate(
            [
                copies[:, cut],
                stack_rows(duals_ref, t),
                jnp.zeros((1, LANES), f32),
                vis_ref[t : t + 1, :].astype(f32),
            ],
            axis=0,
        )
        row = lax.broadcasted_iota(i32, (8, LANES), 0)
        for j in range(per):
            d = t * per + j
            live = jnp.where(lane < counts_ref[0, 0, d], 1.0, 0.0)
            tile = base if j == 0 else pltpu.roll(base, LANES - j * block, 1)
            outgoing[d] = jnp.where(row == 6, live, tile)

    slot_tab = table(copies, LANES)

    def observe(c, acc):
        span = (obs_tiles, c * CHUNK, CHUNK)
        slot = strip(obs_slot_ref, 0, 1, *span)
        at = pick(slot_tab, one_hot(slot & (LANES - 1)), slot >> 7)
        error = strip(meas_ref, 0, 3, *span) - at[0:3]
        pull = None
        for k in range(3):
            term = strip(jac_ref, k * params, params, *span) * error[k : k + 1]
            pull = term if pull is None else pull + term
        pose = strip(obs_pose_ref, 0, 1, *span)
        out = spread(pad_rows(pull, 8), one_hot(pose & (LANES - 1)), pose >> 7, pose_tiles)
        return out if acc is None else acc + out

    pl.semaphore_wait(barrier, robots - 1 + subs - 1)

    first = []
    for k in range(1, robots):
        target = lax.rem(me_r + k, robots)
        copy = pltpu.make_async_remote_copy(
            src_ref=outgoing.at[target], dst_ref=received.at[k],
            send_sem=send1.at[k], recv_sem=recv1.at[k],
            device_id={"robot": target}, device_id_type=MESH,
        )
        copy.start()
        first.append(copy)
    pose_copies = []
    for k in range(1, subs):
        copy = pltpu.make_async_remote_copy(
            src_ref=poses_ref, dst_ref=pose_in.at[k],
            send_sem=sendp.at[k], recv_sem=recvp.at[k],
            device_id={"sub": lax.rem(me_s + k, subs)}, device_id_type=MESH,
        )
        copy.start()
        pose_copies.append(copy)

    chunks = obs_tiles // CHUNK
    half = chunks // 2
    acc = None
    for c in range(half):
        acc = observe(c, acc)

    for copy in first:
        copy.wait()

    group = 8
    totals = None
    entries = []
    for g in range(robots // group):
        blocks = [outgoing[me_r] if k == 0 else received[k] for k in range(g * group, (g + 1) * group)]
        entry = jnp.concatenate(blocks, axis=1)
        ids = entry[7:8].astype(i32)
        live = entry[6:7]
        hot = one_hot(ids & (LANES - 1))
        value = jnp.concatenate(
            [(entry[0:3] + entry[3:6]) * live, live, jnp.zeros((4, entry.shape[1]), f32)], axis=0
        )
        out = spread(value, hot, ids >> 7, tiles)
        totals = out if totals is None else totals + out
        entries.append((entry, hot, ids >> 7))
    new_tiles = []
    dual_part = jnp.zeros((1, LANES), f32)
    for h in range(tiles):
        total = totals[h * 16 : h * 16 + 8] + totals[h * 16 + 8 : h * 16 + 16]
        old = stack_rows(old_ref, h)
        seen = total[3:4]
        fresh = (old + total[0:3]) / (1.0 + seen)
        change = fresh - old
        dual_part += seen * jnp.sum(change * change, axis=0, keepdims=True)
        for a in range(3):
            cons_ref[a, h : h + 1, :] = fresh[a : a + 1]
        new_tiles.append(fresh)
    cons_tab = table(jnp.concatenate(new_tiles, axis=1), LANES)
    primal_part = jnp.zeros((1, LANES), f32)
    fresh_duals = []
    for entry, hot, hi in entries:
        back = pick(cons_tab, hot, hi)[0:3]
        differ = (entry[0:3] - back) * entry[6:7]
        squares = jnp.sum(differ * differ, axis=0, keepdims=True)
        for k in range(group):
            primal_part += squares[:, k * LANES : (k + 1) * LANES]
        fresh_duals.append(entry[3:6] + differ)
    tail = jnp.concatenate([primal_part, penalty * penalty * dual_part, jnp.zeros((3, LANES), f32)], axis=0)
    second = []
    for k in range(robots):
        g, j = divmod(k, group)
        tile = jnp.concatenate([fresh_duals[g][:, j * LANES : (j + 1) * LANES], tail], axis=0)
        if k == 0:
            back_in[me_r] = tile
        else:
            back_out[k] = tile
    for k in range(1, robots):
        copy = pltpu.make_async_remote_copy(
            src_ref=back_out.at[k], dst_ref=back_in.at[me_r],
            send_sem=send2.at[k], recv_sem=recv2.at[k],
            device_id={"robot": lax.rem(me_r + robots - k, robots)}, device_id_type=MESH,
        )
        copy.start()
        second.append(copy)

    for c in range(half, chunks):
        acc = observe(c, acc)

    for copy in second:
        copy.wait()
    part = back_in[0]
    for d in range(1, robots):
        part = part + back_in[d]
    part_out[...] = part
    third = []
    for k in range(1, subs):
        copy = pltpu.make_async_remote_copy(
            src_ref=part_out, dst_ref=part_in.at[k],
            send_sem=send3.at[k], recv_sem=recv3.at[k],
            device_id={"sub": lax.rem(me_s + k, subs)}, device_id_type=MESH,
        )
        copy.start()
        third.append(copy)

    for t in range(slots // LANES):
        tile = back_in[t * per]
        for j in range(1, per):
            moved = pltpu.roll(back_in[t * per + j], j * block, 1)
            tile = jnp.where(lane < j * block, tile, moved)
        for a in range(3):
            dual_ref[a, t : t + 1, :] = tile[a : a + 1]

    for copy in pose_copies:
        copy.wait()
    edge = strip(edge_to_ref, 0, 1, pose_tiles, 0, pose_tiles)
    hot = one_hot(edge & (LANES - 1))
    edge_hi = edge >> 7
    poses = strip(poses_ref, 0, params, pose_tiles, 0, pose_tiles)
    far = None
    for k in range(subs):
        owner = lax.rem(me_s + subs - k, subs)
        source = poses if k == 0 else strip(pose_in, 0, params, pose_tiles, 0, pose_tiles, (k,))
        part_far = pick(table(source, LANES), hot, edge_hi - owner * pose_tiles)
        far = part_far if far is None else far + part_far
    for t in range(pose_tiles):
        cut = slice(t * LANES, (t + 1) * LANES)
        here = poses[:, cut]
        grad = (acc[t * 16 : t * 16 + 8] + acc[t * 16 + 8 : t * 16 + 16] + far[:, cut])[0:params]
        grad = grad - here - strip(edge_off_ref, 0, params, pose_tiles, t, 1)
        for b in range(params):
            column = inv_ref[pl.ds(b * pose_tiles + t, params, stride=params * pose_tiles), :]
            here = here + column * grad[b : b + 1]
        refined_ref[pl.ds(t, params, stride=pose_tiles), :] = here

    for copy in third:
        copy.wait()
    for k in range(1, subs):
        part = part + part_in[k]
    sums = jnp.sum(part, axis=1, keepdims=True)
    norms = jnp.sqrt(sums / float(owned * robots * subs))
    res_ref[...] = jnp.where(lane == 0, norms[3:4], norms[4:5])


def body(*args):
    robots = lax.axis_size("robot")
    subs = lax.axis_size("sub")
    copies, consensus_old, poses = args[0], args[4], args[5]
    flat = [x if i == 3 else x.reshape(x.size // LANES, LANES) for i, x in enumerate(args)]
    for i in (0, 1, 4):
        flat[i] = args[i].reshape(args[i].shape[2], -1, LANES)
    vmem = pl.BlockSpec(memory_space=pltpu.VMEM)
    smem = pl.BlockSpec(memory_space=pltpu.SMEM)
    dma = pltpu.SemaphoreType.DMA
    refined, consensus, dual_new, norms = pl.pallas_call(
        functools.partial(kernel, robots, subs),
        out_shape=(
            jax.ShapeDtypeStruct(flat[5].shape, f32),
            jax.ShapeDtypeStruct(flat[4].shape, f32),
            jax.ShapeDtypeStruct(flat[0].shape, f32),
            jax.ShapeDtypeStruct((1, LANES), f32),
        ),
        in_specs=[smem if i == 3 else vmem for i in range(13)],
        out_specs=(vmem, vmem, vmem, vmem),
        scratch_shapes=[
            pltpu.VMEM((robots, 8, LANES), f32),
            pltpu.VMEM((robots, 8, LANES), f32),
            pltpu.VMEM((robots, 8, LANES), f32),
            pltpu.VMEM((robots, 8, LANES), f32),
            pltpu.VMEM((subs,) + flat[5].shape, f32),
            pltpu.VMEM((8, LANES), f32),
            pltpu.VMEM((subs, 8, LANES), f32),
            dma((robots,)), dma((robots,)), dma((robots,)), dma((robots,)),
            dma((subs,)), dma((subs,)), dma((subs,)), dma((subs,)),
        ],
        compiler_params=pltpu.CompilerParams(collective_id=0, has_side_effects=True),
    )(*flat)
    return (
        refined.reshape(poses.shape),
        consensus.reshape(consensus_old.shape),
        dual_new.reshape(copies.shape),
        norms[0, :2],
    )


def solution(mesh):
    four = P("robot", "sub", None, None)
    three = P("robot", "sub", None)
    return jax.shard_map(
        body,
        mesh=mesh,
        in_specs=(four, four, three, three, four, four, four, four, four, three, three, three, four),
        out_specs=(four, four, four, P()),
        check_vma=False,
    )
```

```python
import functools

import jax
import jax.numpy as jnp
from jax import lax
from jax.experimental import pallas as pl
from jax.experimental.pallas import tpu as pltpu
from jax.sharding import PartitionSpec as P

penalty = 2.0
LANES = 128
CHUNK = 8
MESH = pl.DeviceIdType.MESH
f32, bf16, i32 = jnp.float32, jnp.bfloat16, jnp.int32


def pieces(x):
    hi = x.astype(bf16).astype(f32)
    return hi, x - hi


def pad_rows(x, rows):
    return jnp.concatenate([x, jnp.zeros((rows - x.shape[0], x.shape[1]), x.dtype)], axis=0)


def strip(ref, first, count, tiles, start, length, at=()):
    parts = [
        ref[(*at, pl.ds(first * tiles + t, count, stride=tiles), slice(None))] if count > 1
        else ref[(*at, slice(first * tiles + t, first * tiles + t + 1), slice(None))]
        for t in range(start, start + length)
    ]
    return parts[0] if length == 1 else jnp.concatenate(parts, axis=1)


def stack_rows(ref, t):
    return jnp.concatenate([ref[k, t : t + 1, :] for k in range(ref.shape[0])], axis=0)


def one_hot(lo):
    rows = lax.broadcasted_iota(i32, (LANES, lo.shape[1]), 0)
    return jnp.where(rows == lo, 1.0, 0.0).astype(bf16)


def table(x, width):
    groups = []
    for h in range(x.shape[1] // width):
        hi, lo = pieces(pad_rows(x[:, h * width : (h + 1) * width], 8))
        groups.append(jnp.concatenate([hi, lo], axis=1))
    return jnp.concatenate(groups, axis=0).astype(bf16)


def pick(tab, hot, hi):
    found = jnp.dot(tab, jnp.concatenate([hot, hot], axis=0), preferred_element_type=f32)
    total = None
    for h in range(tab.shape[0] // 8):
        part = jnp.where(hi == h, found[h * 8 : h * 8 + 8], 0.0)
        total = part if total is None else total + part
    return total


def spread(values, hot, hi, tiles):
    a, b = pieces(values)
    both = jnp.concatenate([a, b], axis=0)
    lhs = jnp.concatenate([jnp.where(hi == h, both, 0.0) for h in range(tiles)], axis=0).astype(bf16)
    return lax.dot_general(lhs, hot, (((1,), (1,)), ((), ())), preferred_element_type=f32)


def kernel(robots, subs, *refs):
    sources, refs = refs[:13], refs[13:]
    (refined_ref, cons_ref, dual_ref, res_ref), refs = refs[:4], refs[4:]
    staged, refs = refs[:13], refs[13:]
    (
        copies_ref, duals_ref, vis_ref, counts_ref, old_ref, poses_ref, inv_ref, jac_ref, meas_ref,
        obs_pose_ref, obs_slot_ref, edge_to_ref, edge_off_ref,
    ) = staged
    (
        outgoing, received, back_out, back_in, pose_in, part_out, part_in,
        load_sem, send1, recv1, send2, recv2, sendp, recvp, send3, recv3,
    ) = refs
    me_r = lax.axis_index("robot")
    me_s = lax.axis_index("sub")
    slot_tiles = vis_ref.shape[0]
    slots = slot_tiles * LANES
    block = slots // robots
    per = LANES // block
    tiles = old_ref.shape[1]
    owned = tiles * LANES
    pose_tiles = edge_to_ref.shape[0]
    obs_tiles = obs_slot_ref.shape[0]
    params = poses_ref.shape[0] // pose_tiles
    robot_steps = sorted(range(1, robots), key=lambda k: -min(k, robots - k))

    barrier = pltpu.get_barrier_semaphore()
    peers = [(kr, ks) for kr in [*robot_steps, 0] for ks in range(subs) if (kr, ks) != (0, 0)]
    for kr, ks in peers:
        there = (lax.rem(me_r + kr, robots), lax.rem(me_s + ks, subs))
        pl.semaphore_signal(barrier, inc=1, device_id=there, device_id_type=MESH)

    loads = [pltpu.make_async_copy(sources[i], staged[i], load_sem.at[i]) for i in range(13)]
    order = (0, 1, 2, 3, 10, 8, 7, 9, 5, 4, 11, 12, 6)
    for i in order:
        loads[i].start()

    lane = lax.broadcasted_iota(i32, (1, LANES), 1)
    row = lax.broadcasted_iota(i32, (8, LANES), 0)
    my_part = lax.rem(me_r, per)
    for i in order[:4]:
        loads[i].wait()
    copies = jnp.concatenate([stack_rows(copies_ref, t) for t in range(slot_tiles)], axis=1)
    for t in range(slot_tiles):
        cut = slice(t * LANES, (t + 1) * LANES)
        base = jnp.concatenate(
            [copies[:, cut], stack_rows(duals_ref, t), jnp.zeros((1, LANES), f32), vis_ref[t : t + 1, :].astype(f32)],
            axis=0,
        )
        for j in range(per):
            d = t * per + j
            tile = base
            for p in range(per):
                if p != j:
                    moved = pltpu.roll(base, (p - j) * block % LANES, 1)
                    tile = jnp.where(my_part == p, moved, tile)
            live = jnp.where(lane - my_part * block < counts_ref[0, 0, d], 1.0, 0.0)
            outgoing[d] = jnp.where(row == 6, live, tile)

    slot_tab = table(copies, LANES)
    for i in order[4:]:
        loads[i].wait()

    def observe(c, acc):
        span = (obs_tiles, c * CHUNK, CHUNK)
        slot = strip(obs_slot_ref, 0, 1, *span)
        at = pick(slot_tab, one_hot(slot & (LANES - 1)), slot >> 7)
        error = strip(meas_ref, 0, 3, *span) - at[0:3]
        pull = None
        for k in range(3):
            term = strip(jac_ref, k * params, params, *span) * error[k : k + 1]
            pull = term if pull is None else pull + term
        pose = strip(obs_pose_ref, 0, 1, *span)
        out = spread(pad_rows(pull, 8), one_hot(pose & (LANES - 1)), pose >> 7, pose_tiles)
        return out if acc is None else acc + out

    acc = None
    for c in range(obs_tiles // CHUNK):
        acc = observe(c, acc)

    edge = strip(edge_to_ref, 0, 1, pose_tiles, 0, pose_tiles)
    edge_hot = one_hot(edge & (LANES - 1))
    edge_hi = edge >> 7
    poses = strip(poses_ref, 0, params, pose_tiles, 0, pose_tiles)
    far = pick(table(poses, LANES), edge_hot, edge_hi - me_s * pose_tiles)
    grads = []
    for t in range(pose_tiles):
        cut = slice(t * LANES, (t + 1) * LANES)
        grad = (acc[t * 16 : t * 16 + 8] + acc[t * 16 + 8 : t * 16 + 16] + far[:, cut])[0:params]
        grads.append(grad - poses[:, cut] - strip(edge_off_ref, 0, params, pose_tiles, t, 1))
    grad = jnp.concatenate(grads, axis=1)

    pl.semaphore_wait(barrier, len(peers))

    first = []
    for k in robot_steps:
        target = lax.rem(me_r + k, robots)
        copy = pltpu.make_async_remote_copy(
            src_ref=outgoing.at[target], dst_ref=received.at[k],
            send_sem=send1.at[k], recv_sem=recv1.at[k],
            device_id={"robot": target}, device_id_type=MESH,
        )
        copy.start()
        first.append(copy)
    pose_copies = []
    for k in range(1, subs):
        copy = pltpu.make_async_remote_copy(
            src_ref=poses_ref, dst_ref=pose_in.at[k],
            send_sem=sendp.at[k], recv_sem=recvp.at[k],
            device_id={"sub": lax.rem(me_s + k, subs)}, device_id_type=MESH,
        )
        copy.start()
        pose_copies.append(copy)

    for copy in first:
        copy.wait_recv()

    merged = []
    for g in range(robots // per):
        tile = None
        for j in range(per):
            k = g * per + j
            one = outgoing[me_r] if k == 0 else received[k]
            place = lax.rem(me_r + robots - k, per)
            mine = lane >= place * block
            tile = one if tile is None else jnp.where(mine & (lane < place * block + block), one, tile)
        merged.append(tile)
    group = min(8, len(merged))
    totals = None
    entries = []
    for g in range(0, len(merged), group):
        entry = jnp.concatenate(merged[g : g + group], axis=1)
        ids = entry[7:8].astype(i32)
        live = entry[6:7]
        hot = one_hot(ids & (LANES - 1))
        value = jnp.concatenate(
            [(entry[0:3] + entry[3:6]) * live, live, jnp.zeros((4, entry.shape[1]), f32)], axis=0
        )
        out = spread(value, hot, ids >> 7, tiles)
        totals = out if totals is None else totals + out
        entries.append((entry, hot, ids >> 7))
    new_tiles = []
    dual_part = jnp.zeros((1, LANES), f32)
    for h in range(tiles):
        total = totals[h * 16 : h * 16 + 8] + totals[h * 16 + 8 : h * 16 + 16]
        old = stack_rows(old_ref, h)
        seen = total[3:4]
        fresh = (old + total[0:3]) / (1.0 + seen)
        change = fresh - old
        dual_part += seen * jnp.sum(change * change, axis=0, keepdims=True)
        for a in range(3):
            cons_ref[a, h : h + 1, :] = fresh[a : a + 1]
        new_tiles.append(fresh)
    cons_tab = table(jnp.concatenate(new_tiles, axis=1), LANES)
    primal_part = jnp.zeros((1, LANES), f32)
    g = 0
    for entry, hot, hi in entries:
        back = pick(cons_tab, hot, hi)[0:3]
        differ = (entry[0:3] - back) * entry[6:7]
        squares = jnp.sum(differ * differ, axis=0, keepdims=True)
        fresh_dual = pad_rows(entry[3:6] + differ, 8)
        for k in range(entry.shape[1] // LANES):
            cut = slice(k * LANES, (k + 1) * LANES)
            primal_part += squares[:, cut]
            back_out[g] = fresh_dual[:, cut]
            g += 1
    part = jnp.concatenate([primal_part, penalty * penalty * dual_part], axis=0)
    part_out[...] = part
    back_in[me_r] = back_out[0]

    second = []
    for k in robot_steps:
        copy = pltpu.make_async_remote_copy(
            src_ref=back_out.at[k // per], dst_ref=back_in.at[me_r],
            send_sem=send2.at[k], recv_sem=recv2.at[k],
            device_id={"robot": lax.rem(me_r + robots - k, robots)}, device_id_type=MESH,
        )
        copy.start()
        second.append(copy)
    third = []
    for kr, ks in peers:
        n = kr * subs + ks
        copy = pltpu.make_async_remote_copy(
            src_ref=part_out, dst_ref=part_in.at[n],
            send_sem=send3.at[n], recv_sem=recv3.at[n],
            device_id=(lax.rem(me_r + kr, robots), lax.rem(me_s + ks, subs)), device_id_type=MESH,
        )
        copy.start()
        third.append(copy)

    for copy in pose_copies:
        copy.wait()
    for k in range(1, subs):
        owner = lax.rem(me_s + subs - k, subs)
        source = strip(pose_in, 0, params, pose_tiles, 0, pose_tiles, (k,))
        grad = grad + pick(table(source, LANES), edge_hot, edge_hi - owner * pose_tiles)[0:params]
    for t in range(pose_tiles):
        cut = slice(t * LANES, (t + 1) * LANES)
        here = poses[:, cut]
        for b in range(params):
            column = inv_ref[pl.ds(b * pose_tiles + t, params, stride=params * pose_tiles), :]
            here = here + column * grad[b : b + 1, cut]
        refined_ref[pl.ds(t, params, stride=pose_tiles), :] = here

    for copy in first:
        copy.wait_send()
    for copy in second:
        copy.wait()
    for t in range(slot_tiles):
        tile = None
        for j in range(per):
            raw = back_in[t * per + j]
            one = raw
            for p in range(per):
                if p != j:
                    moved = pltpu.roll(raw, (j - p) * block % LANES, 1)
                    one = jnp.where(my_part == p, moved, one)
            tile = one if tile is None else jnp.where(lane < j * block, tile, one)
        for a in range(3):
            dual_ref[a, t : t + 1, :] = tile[a : a + 1]

    for copy in third:
        copy.wait()
    for kr, ks in peers:
        part = part + part_in[kr * subs + ks]
    sums = jnp.sum(part, axis=1, keepdims=True)
    norms = jnp.sqrt(sums / float(owned * robots * subs))
    res_ref[...] = jnp.where(lane == 0, norms[0:1], norms[1:2])


def write_out(refined, consensus, dual_new, norms, refined_ref, cons_ref, dual_ref, res_ref):
    refined_ref[...] = refined[...]
    cons_ref[...] = consensus[...]
    dual_ref[...] = dual_new[...]
    res_ref[...] = norms[0, 0:2]


def body(*args):
    robots = lax.axis_size("robot")
    subs = lax.axis_size("sub")
    copies, consensus_old, poses = args[0], args[4], args[5]
    flat = [x if i == 3 else x.reshape(x.size // LANES, LANES) for i, x in enumerate(args)]
    for i in (0, 1, 4):
        flat[i] = args[i].reshape(args[i].shape[2], -1, LANES)
    vmem = pl.BlockSpec(memory_space=pltpu.VMEM)
    dma = pltpu.SemaphoreType.DMA
    everyone = robots * subs
    shapes = [flat[5].shape, flat[4].shape, flat[0].shape]
    held = pl.pallas_call(
        functools.partial(kernel, robots, subs),
        out_shape=tuple(pltpu.VMEM(shape, f32) for shape in [*shapes, (1, LANES)]),
        in_specs=[pl.BlockSpec(memory_space=pl.ANY)] * 13,
        out_specs=(vmem,) * 4,
        scratch_shapes=[
            *[(pltpu.SMEM if i == 3 else pltpu.VMEM)(x.shape, x.dtype) for i, x in enumerate(flat)],
            pltpu.VMEM((robots, 8, LANES), f32),
            pltpu.VMEM((robots, 8, LANES), f32),
            pltpu.VMEM((robots, 8, LANES), f32),
            pltpu.VMEM((robots, 8, LANES), f32),
            pltpu.VMEM((subs,) + flat[5].shape, f32),
            pltpu.VMEM((2, LANES), f32),
            pltpu.VMEM((everyone, 2, LANES), f32),
            dma((13,)),
            dma((robots,)), dma((robots,)), dma((robots,)), dma((robots,)),
            dma((subs,)), dma((subs,)), dma((everyone,)), dma((everyone,)),
        ],
        compiler_params=pltpu.CompilerParams(collective_id=0, has_side_effects=True),
    )(*flat)
    refined, consensus, dual_new, norms = pl.pallas_call(
        write_out,
        out_shape=tuple(jax.ShapeDtypeStruct(shape, f32) for shape in [*shapes, (2,)]),
        in_specs=[vmem] * 4,
        out_specs=(vmem,) * 4,
    )(*[pltpu.with_memory_space_constraint(x, pltpu.VMEM) for x in held])
    return (
        refined.reshape(poses.shape),
        consensus.reshape(consensus_old.shape),
        dual_new.reshape(copies.shape),
        norms,
    )


def solution(mesh):
    four = P("robot", "sub", None, None)
    three = P("robot", "sub", None)
    return jax.shard_map(
        body,
        mesh=mesh,
        in_specs=(four, four, three, three, four, four, four, four, four, three, three, three, four),
        out_specs=(four, four, four, P()),
        check_vma=False,
    )
```
